128 devices in a mesh: z: 4 (over z), y: 4 (over y), x: 8 (over x, core).
Axes of the slice: x: 4, y: 4, z: 4, core: 2. Of those that a mesh axis runs over, the one named last changes fastest.
Arguments:
- x_in: bfloat16 [131072, 2048], P(('z', 'y', 'x'))
- g_out: bfloat16 [131072, 256], P(('z', 'y', 'x'))
- w_in: bfloat16 [2048, 256], replicated
- w_up1: bfloat16 [256, 1024], replicated
- w_down1: bfloat16 [1024, 256], replicated
- w_up2: bfloat16 [256, 1024], replicated
- w_down2: bfloat16 [1024, 256], replicated
Outputs:
- output 1: bfloat16 [131072, 2048], P(('z', 'y', 'x'))
- output 2: float32 [2048, 256], replicated
- output 3: float32 [256, 1024], replicated
- output 4: float32 [1024, 256], replicated
- output 5: float32 [256, 1024], replicated
- output 6: float32 [1024, 256], replicated
All inputs are finite; a program needn't handle non-finite values.
Results may differ from the reference program's by a relative error of at most 0.0133384.
Values are sent between devices in bfloat16 or wider.
A program may use at most 1 GiB of HBM per device.

```python
import jax
import jax.numpy as jnp
from jax import lax

D_MODEL = 256
D_FF = 1024
D_IN = 2048
TOK_DEV = 1024
N_DEVICES = 128

TOKENS = TOK_DEV * N_DEVICES
SQRT_HALF = 0.7071067811865476
INV_SQRT_TAU = 0.3989422804014327


def gelu_value(pre_act):
    pre_wide = pre_act.astype(jnp.float32)
    return 0.5 * pre_wide * (1.0 + lax.erf(pre_wide * SQRT_HALF))


def gelu_slope(pre_act):
    pre_wide = pre_act.astype(jnp.float32)
    return 0.5 * (1.0 + lax.erf(pre_wide * SQRT_HALF)) + pre_wide * jnp.exp(-0.5 * pre_wide * pre_wide) * INV_SQRT_TAU


def setup_inputs(seed: int = 0) -> dict:
    keys = jax.random.split(jax.random.key(seed), 7)
    x_in = jax.random.normal(keys[0], (TOKENS, D_IN), jnp.float32)
    g_out = jax.random.normal(keys[1], (TOKENS, D_MODEL), jnp.float32)
    w_in = jax.random.normal(keys[2], (D_IN, D_MODEL), jnp.float32) * D_IN ** -0.5
    w_up1 = jax.random.normal(keys[3], (D_MODEL, D_FF), jnp.float32) * D_MODEL ** -0.5
    w_down1 = jax.random.normal(keys[4], (D_FF, D_MODEL), jnp.float32) * D_FF ** -0.5
    w_up2 = jax.random.normal(keys[5], (D_MODEL, D_FF), jnp.float32) * D_MODEL ** -0.5
    w_down2 = jax.random.normal(keys[6], (D_FF, D_MODEL), jnp.float32) * D_FF ** -0.5
    return {
        "x_in": x_in.astype(jnp.bfloat16),
        "g_out": g_out.astype(jnp.bfloat16),
        "w_in": w_in.astype(jnp.bfloat16),
        "w_up1": w_up1.astype(jnp.bfloat16),
        "w_down1": w_down1.astype(jnp.bfloat16),
        "w_up2": w_up2.astype(jnp.bfloat16),
        "w_down2": w_down2.astype(jnp.bfloat16),
    }


def local_backward(x_in, g_out, w_in, w_up1, w_down1, w_up2, w_down2):
    x_mid = jnp.dot(x_in, w_in, preferred_element_type=jnp.float32).astype(jnp.bfloat16)
    pre_one = jnp.dot(x_mid, w_up1, preferred_element_type=jnp.float32).astype(jnp.bfloat16)
    act_one = gelu_value(pre_one).astype(jnp.bfloat16)
    hid_two = (jnp.dot(act_one, w_down1, preferred_element_type=jnp.float32) + x_mid.astype(jnp.float32)).astype(jnp.bfloat16)
    pre_three = jnp.dot(hid_two, w_up2, preferred_element_type=jnp.float32).astype(jnp.bfloat16)
    act_three = gelu_value(pre_three).astype(jnp.bfloat16)
    grad_down2 = jnp.dot(act_three.T, g_out, preferred_element_type=jnp.float32)
    d_act3 = jnp.dot(g_out, w_down2.T, preferred_element_type=jnp.float32).astype(jnp.bfloat16)
    d_pre3 = (d_act3.astype(jnp.float32) * gelu_slope(pre_three)).astype(jnp.bfloat16)
    grad_up2 = jnp.dot(hid_two.T, d_pre3, preferred_element_type=jnp.float32)
    d_hid2 = (jnp.dot(d_pre3, w_up2.T, preferred_element_type=jnp.float32) + g_out.astype(jnp.float32)).astype(jnp.bfloat16)
    grad_down1 = jnp.dot(act_one.T, d_hid2, preferred_element_type=jnp.float32)
    d_act1 = jnp.dot(d_hid2, w_down1.T, preferred_element_type=jnp.float32).astype(jnp.bfloat16)
    d_pre1 = (d_act1.astype(jnp.float32) * gelu_slope(pre_one)).astype(jnp.bfloat16)
    grad_up1 = jnp.dot(x_mid.T, d_pre1, preferred_element_type=jnp.float32)
    d_mid = (jnp.dot(d_pre1, w_up1.T, preferred_element_type=jnp.float32) + d_hid2.astype(jnp.float32)).astype(jnp.bfloat16)
    grad_in = jnp.dot(x_in.T, d_mid, preferred_element_type=jnp.float32)
    dx_rows = jnp.dot(d_mid, w_in.T, preferred_element_type=jnp.float32).astype(jnp.bfloat16)
    return dx_rows, (grad_in, grad_up1, grad_down1, grad_up2, grad_down2)


def reference(x_in, g_out, w_in, w_up1, w_down1, w_up2, w_down2):
    x_shards = x_in.reshape(N_DEVICES, TOK_DEV, D_IN)
    g_shards = g_out.reshape(N_DEVICES, TOK_DEV, D_MODEL)
    zero_sums = (
        jnp.zeros((D_IN, D_MODEL), jnp.float32),
        jnp.zeros((D_MODEL, D_FF), jnp.float32),
        jnp.zeros((D_FF, D_MODEL), jnp.float32),
        jnp.zeros((D_MODEL, D_FF), jnp.float32),
        jnp.zeros((D_FF, D_MODEL), jnp.float32),
    )

    def shard_step(partial_sums, shard):
        dx_rows, grads = local_backward(shard[0], shard[1], w_in, w_up1, w_down1, w_up2, w_down2)
        return tuple(total + piece for total, piece in zip(partial_sums, grads)), dx_rows

    totals, dx_parts = lax.scan(shard_step, zero_sums, (x_shards, g_shards))
    scale = 1.0 / N_DEVICES
    return (dx_parts.reshape(TOKENS, D_IN), totals[0] * scale, totals[1] * scale, totals[2] * scale, totals[3] * scale, totals[4] * scale)
```

```python
import math
import jax
import jax.numpy as jnp
from jax import lax
from jax.experimental import pallas as pl
from jax.experimental.pallas import tpu as pltpu
from jax.sharding import PartitionSpec as P

SQRT_HALF = 0.7071067811865476
INV_SQRT_TAU = 0.3989422804014327
MESH = pl.DeviceIdType.MESH
RING = 4
UNITS = (
    (0, 0, 1024, 256),
    (1, 0, 256, 1024),
    (2, 0, 1024, 256),
    (3, 0, 256, 1024),
    (4, 0, 1024, 256),
    (4, 1024, 1024, 256),
)
SHAPES = ((1024, 256), (256, 1024), (1024, 256), (256, 1024), (2048, 256))
ORDERS = (("x", "y", "z"), ("y", "z", "x"), ("z", "x", "y"))


def gelu_value(pre_act):
    pre_wide = pre_act.astype(jnp.float32)
    return 0.5 * pre_wide * (1.0 + lax.erf(pre_wide * SQRT_HALF))


def gelu_slope(pre_act):
    pre_wide = pre_act.astype(jnp.float32)
    return 0.5 * (1.0 + lax.erf(pre_wide * SQRT_HALF)) + pre_wide * jnp.exp(-0.5 * pre_wide * pre_wide) * INV_SQRT_TAU


def plain_product(first_op, second_op):
    return lax.dot_general(first_op, second_op, (((1,), (0,)), ((), ())), preferred_element_type=jnp.float32)


def rows_contract(first_op, second_op):
    return lax.dot_general(first_op, second_op, (((0,), (0,)), ((), ())), preferred_element_type=jnp.float32)


def times_transposed(first_op, second_op):
    return lax.dot_general(first_op, second_op, (((1,), (1,)), ((), ())), preferred_element_type=jnp.float32)


def hinted(value, step):
    return value if isinstance(value, int) else pl.multiple_of(value, step)


class Region:
    def __init__(self, row, rows, col, cols):
        self.row, self.rows, self.col, self.cols = row, rows, col, cols

    def at(self, ref):
        return ref.at[pl.ds(hinted(self.row, 8), self.rows), pl.ds(hinted(self.col, 128), self.cols)]

    def load(self, ref):
        return ref[pl.ds(hinted(self.row, 8), self.rows), pl.ds(hinted(self.col, 128), self.cols)]

    def store(self, ref, value):
        ref[pl.ds(hinted(self.row, 8), self.rows), pl.ds(hinted(self.col, 128), self.cols)] = value

    def part(self, index, count):
        if self.rows // count >= 8:
            step = self.rows // count
            return Region(self.row + index * step, step, self.col, self.cols)
        step = self.cols // count
        return Region(self.row, self.rows, self.col + index * step, step)

    def shape(self):
        return (self.rows, self.cols)

    def moved(self, row, col):
        return Region(self.row + row, self.rows, self.col + col, self.cols)


class Semaphores:
    def __init__(self, send, recv):
        self.send, self.recv, self.used, self.copies = send, recv, 0, []

    def copy(self, source, target, device):
        number = self.used
        self.used += 1
        made = pltpu.make_async_remote_copy(
            src_ref=source,
            dst_ref=target,
            send_sem=self.send.at[number],
            recv_sem=self.recv.at[number],
            device_id=device,
            device_id_type=MESH,
        )
        made.start()
        self.copies.append(made)
        return made


def place():
    x = lax.axis_index("x")
    return {"x": x // 2, "y": lax.axis_index("y"), "z": lax.axis_index("z"), "core": lax.rem(x, 2)}


def neighbour(here, axis, step):
    other = lax.rem(here[axis] + step + RING, RING)
    return {"x": other * 2 + here["core"]} if axis == "x" else {axis: other}


def partner(here):
    return {"x": here["x"] * 2 + 1 - here["core"]}


def greet(here):
    barrier = pltpu.get_barrier_semaphore()
    peers = [partner(here)]
    for axis in ("x", "y", "z"):
        peers += [neighbour(here, axis, 1), neighbour(here, axis, -1)]
    for peer in peers:
        pl.semaphore_signal(barrier, inc=1, device_id=peer, device_id_type=MESH)
    pl.semaphore_wait(barrier, len(peers))


def buffer_shapes(rows, cols):
    half = Region(0, rows, 0, cols).part(0, 2)
    shapes = [half.shape(), half.shape()]
    block = half
    for _ in range(3):
        block = block.part(0, RING)
        piece = block.part(0, 2)
        shapes += [piece.shape(), piece.shape(), block.shape(), block.shape()]
    return shapes


def reduce_unit(here, order, grad, whole, buffers, out, sems, scale):
    core = here["core"]
    far = partner(here)
    from_pair, total = buffers[0], buffers[1]
    pair = sems.copy(whole.part(1 - core, 2).at(grad), from_pair, far)
    yield
    pair.wait_recv()
    mine = whole.part(core, 2)
    total[...] = mine.load(grad) + from_pair[...]
    base = Region(0, mine.rows, 0, mine.cols)
    levels = []
    for level, axis in enumerate(order):
        from_left_far, from_right_far, from_left, from_right = buffers[2 + 4 * level : 6 + 4 * level]
        at = here[axis]
        right, left = neighbour(here, axis, 1), neighbour(here, axis, -1)
        shard = [base.part(lax.rem(at + step, RING), RING) for step in range(RING)]
        local = Region(0, shard[0].rows, 0, shard[0].cols)
        first, second = local.part(0, 2), local.part(1, 2)
        far_right = sems.copy(shard[2].part(0, 2).at(total), from_left_far, right)
        far_left = sems.copy(shard[2].part(1, 2).at(total), from_right_far, left)
        near_right = sems.copy(shard[1].part(1, 2).at(total), second.at(from_left), right)
        near_left = sems.copy(shard[3].part(0, 2).at(total), first.at(from_right), left)
        yield
        far_right.wait_recv()
        block = shard[1].part(0, 2)
        block.store(total, block.load(total) + from_left_far[...])
        sum_right = sems.copy(block.at(total), first.at(from_left), right)
        far_left.wait_recv()
        block = shard[3].part(1, 2)
        block.store(total, block.load(total) + from_right_far[...])
        sum_left = sems.copy(block.at(total), second.at(from_right), left)
        yield
        for copy in (near_right, near_left, sum_right, sum_left):
            copy.wait_recv()
        result = shard[0].load(total) + (from_left[...] + from_right[...])
        if level < 2:
            shard[0].store(total, result)
        else:
            shard[0].moved(mine.row, mine.col).store(out, result * scale)
        levels.append((shard, right, left))
        base = shard[0]
    for level in (2, 1, 0):
        shard, right, left = levels[level]
        shard = [block.moved(mine.row, mine.col) for block in shard]
        halves = [(block.part(0, 2).at(out), block.part(1, 2).at(out)) for block in shard]
        own_first, own_second = halves[0]
        right_first = sems.copy(own_first, own_first, right)
        left_second = sems.copy(own_second, own_second, left)
        right_second = sems.copy(own_second, own_second, right)
        left_first = sems.copy(own_first, own_first, left)
        if level == 0:
            pair_copies = [sems.copy(shard[0].at(out), shard[0].at(out), far)]
        yield
        right_first.wait_recv()
        pass_right = sems.copy(halves[3][0], halves[3][0], right)
        left_second.wait_recv()
        pass_left = sems.copy(halves[1][1], halves[1][1], left)
        yield
        right_second.wait_recv()
        left_first.wait_recv()
        if level == 0:
            pair_copies += [sems.copy(shard[step].at(out), shard[step].at(out), far) for step in (1, 3)]
            yield
        pass_right.wait_recv()
        pass_left.wait_recv()
        if level == 0:
            pair_copies.append(sems.copy(shard[2].at(out), shard[2].at(out), far))
    yield
    for copy in pair_copies:
        copy.wait_recv()


COPIES = 1 + 3 * 6 + 3 * 6 + 4


def reduce_kernel(scale, *refs):
    grads, refs = refs[:5], refs[5:]
    outs, refs = refs[:5], refs[5:]
    send, recv = refs[-2:]
    here = place()
    greet(here)
    sems = Semaphores(send, recv)
    running = []
    at = 0
    for number, (array, row, rows, cols) in enumerate(UNITS):
        count = len(buffer_shapes(rows, cols))
        running.append(
            reduce_unit(here, ORDERS[number % 3], grads[array], Region(row, rows, 0, cols), refs[at : at + count], outs[array], sems, scale)
        )
        at += count
    while running:
        for unit in list(running):
            if next(unit, "done") == "done":
                running.remove(unit)
    for copy in sems.copies:
        copy.wait_send()


def all_reduce(grads, scale):
    scratch = []
    for _, _, rows, cols in UNITS:
        scratch += [pltpu.VMEM(shape, jnp.float32) for shape in buffer_shapes(rows, cols)]
    scratch += [pltpu.SemaphoreType.DMA((COPIES * len(UNITS),))] * 2
    vmem = pl.BlockSpec(memory_space=pltpu.VMEM)

    def body(*refs):
        reduce_kernel(scale, *refs)

    return pl.pallas_call(
        body,
        out_shape=[jax.ShapeDtypeStruct(shape, jnp.float32) for shape in SHAPES],
        in_specs=[vmem] * 5,
        out_specs=[vmem] * 5,
        scratch_shapes=scratch,
        compiler_params=pltpu.CompilerParams(collective_id=0, has_side_effects=True, vmem_limit_bytes=48 * 1024 * 1024),
    )(*grads)


def solution(mesh):
    batch_axes = ("z", "y", "x")
    device_count = math.prod(mesh.shape.values())
    scale = 1.0 / device_count
    row_spec = P(batch_axes, None)
    full_spec = P(None, None)

    def device_step(x_in, g_out, w_in, w_up1, w_down1, w_up2, w_down2):
        x_mid = plain_product(x_in, w_in).astype(jnp.bfloat16)
        pre_one = plain_product(x_mid, w_up1).astype(jnp.bfloat16)
        act_one = gelu_value(pre_one).astype(jnp.bfloat16)
        hid_two = (plain_product(act_one, w_down1) + x_mid.astype(jnp.float32)).astype(jnp.bfloat16)
        pre_three = plain_product(hid_two, w_up2).astype(jnp.bfloat16)
        act_three = gelu_value(pre_three).astype(jnp.bfloat16)
        dw_down2 = rows_contract(act_three, g_out)
        d_act3 = times_transposed(g_out, w_down2).astype(jnp.bfloat16)
        d_pre3 = (d_act3.astype(jnp.float32) * gelu_slope(pre_three)).astype(jnp.bfloat16)
        dw_up2 = rows_contract(hid_two, d_pre3)
        d_hid2 = (times_transposed(d_pre3, w_up2) + g_out.astype(jnp.float32)).astype(jnp.bfloat16)
        dw_down1 = rows_contract(act_one, d_hid2)
        d_act1 = times_transposed(d_hid2, w_down1).astype(jnp.bfloat16)
        d_pre1 = (d_act1.astype(jnp.float32) * gelu_slope(pre_one)).astype(jnp.bfloat16)
        dw_up1 = rows_contract(x_mid, d_pre1)
        d_mid = (times_transposed(d_pre1, w_up1) + d_hid2.astype(jnp.float32)).astype(jnp.bfloat16)
        dw_in = rows_contract(x_in, d_mid)
        dx_rows = times_transposed(d_mid, w_in).astype(jnp.bfloat16)
        dw_down2, dw_up2, dw_down1, dw_up1, dw_in = all_reduce((dw_down2, dw_up2, dw_down1, dw_up1, dw_in), scale)
        return dx_rows, dw_in, dw_up1, dw_down1, dw_up2, dw_down2

    return jax.shard_map(
        device_step,
        mesh=mesh,
        in_specs=(row_spec, row_spec, full_spec, full_spec, full_spec, full_spec, full_spec),
        out_specs=(row_spec, full_spec, full_spec, full_spec, full_spec, full_spec),
        check_vma=False,
    )
```

```python
import itertools
import math
import jax
import jax.numpy as jnp
from jax import lax
from jax.experimental import pallas as pl
from jax.experimental.pallas import tpu as pltpu
from jax.sharding import PartitionSpec as P

SQRT_HALF = 0.7071067811865476
INV_SQRT_TAU = 0.3989422804014327
MESH = pl.DeviceIdType.MESH
RING = 4
ROWS = 1024
TILE = 512
HALF, WIDE = jnp.bfloat16, jnp.float32
IN, UP1, DOWN1, UP2, DOWN2 = range(5)
SHAPES = ((2048, 256), (256, 1024), (1024, 256), (256, 1024), (1024, 256))
ORDERS = ((("x",), ("y", "z")), (("y",), ("z", "x")), (("z",), ("x", "y")))


def gelu_pair(pre_act):
    wide = pre_act.astype(WIDE)
    share = 0.5 * (1.0 + lax.erf(wide * SQRT_HALF))
    return wide * share, share + wide * jnp.exp(-0.5 * wide * wide) * INV_SQRT_TAU


def plain_product(first_op, second_op):
    return lax.dot_general(first_op, second_op, (((1,), (0,)), ((), ())), preferred_element_type=jnp.float32)


def rows_contract(first_op, second_op):
    return lax.dot_general(first_op, second_op, (((0,), (0,)), ((), ())), preferred_element_type=jnp.float32)


def times_transposed(first_op, second_op):
    return lax.dot_general(first_op, second_op, (((1,), (1,)), ((), ())), preferred_element_type=jnp.float32)


def hinted(value, step):
    return value if isinstance(value, int) else pl.multiple_of(value, step)


class Region:
    def __init__(self, row, rows, col, cols):
        self.row, self.rows, self.col, self.cols = row, rows, col, cols

    def at(self, ref):
        return ref.at[pl.ds(hinted(self.row, 8), self.rows), pl.ds(hinted(self.col, 128), self.cols)]

    def load(self, ref):
        return ref[pl.ds(hinted(self.row, 8), self.rows), pl.ds(hinted(self.col, 128), self.cols)]

    def store(self, ref, value):
        ref[pl.ds(hinted(self.row, 8), self.rows), pl.ds(hinted(self.col, 128), self.cols)] = value

    def part(self, index, count):
        if self.rows // count >= 8:
            step = self.rows // count
            return Region(self.row + index * step, step, self.col, self.cols)
        step = self.cols // count
        if step >= 128:
            return Region(self.row, self.rows, self.col + index * step, step)
        rows, cols = self.rows // 2, self.cols // (count // 2)
        across = self.cols // cols
        return Region(self.row + index // across * rows, rows, self.col + lax.rem(index, across) * cols, cols)

    def shape(self):
        return (self.rows, self.cols)

    def moved(self, row, col):
        return Region(self.row + row, self.rows, self.col + col, self.cols)


class Semaphores:
    def __init__(self, send, recv):
        self.send, self.recv, self.sends, self.recvs, self.closing = send, recv, 0, 0, []

    def stage(self, span):
        number = self.sends
        self.sends += 1
        self.closing.append((number, span))
        return number

    def arrival(self):
        self.recvs += 1
        return self.recvs - 1

    def copy(self, source, target, device, stage, arrival):
        pltpu.make_async_remote_copy(
            src_ref=source,
            dst_ref=target,
            send_sem=self.send.at[stage],
            recv_sem=self.recv.at[arrival],
            device_id=device,
            device_id_type=MESH,
        ).start()

    def arrived(self, arrival, span):
        pltpu.make_async_copy(span, span, self.recv.at[arrival]).wait()

    def close(self):
        for number, span in self.closing:
            pltpu.make_async_copy(span, span, self.send.at[number]).wait()


def place():
    x = lax.axis_index("x")
    return {"x": x // 2, "y": lax.axis_index("y"), "z": lax.axis_index("z"), "core": lax.rem(x, 2)}


def device_at(here, offsets):
    where = {}
    for axis, step in offsets:
        other = lax.rem(here[axis] + step, RING)
        where[axis] = other * 2 + here["core"] if axis == "x" else other
    return where


def partner(here):
    return {"x": here["x"] * 2 + 1 - here["core"]}


def group_offsets(axes):
    steps = list(itertools.product(range(RING), repeat=len(axes)))[1:]
    steps.sort(key=lambda step: -sum(min(s, RING - s) for s in step))
    return steps


def greet(here, groups):
    barrier = pltpu.get_barrier_semaphore()
    peers = {(("core", 1),): partner(here)}
    for axes in groups:
        for step in group_offsets(axes):
            key = tuple(sorted((axis, s) for axis, s in zip(axes, step) if s))
            peers[key] = device_at(here, key)
    for peer in peers.values():
        pl.semaphore_signal(barrier, inc=1, device_id=peer, device_id_type=MESH)
    return len(peers)


def shard_of(block, here, axes, step):
    for axis, s in zip(axes, step):
        block = block.part(lax.rem(here[axis] + s, RING) if s else here[axis], RING)
    return block


def buffer_shapes(half, levels):
    block = half(0)
    shapes = [block.shape(), block.shape()]
    for axes in levels:
        for _ in axes:
            block = block.part(0, RING)
        shapes.append((RING ** len(axes) - 1,) + block.shape())
    return shapes


def reduce_unit(here, levels, grad, half, buffers, out, sems, scale):
    core = here["core"]
    far = partner(here)
    from_pair, total = buffers[0], buffers[1]
    arrival = sems.arrival()
    sems.copy(grad, from_pair, far, sems.stage(from_pair), arrival)
    yield
    sems.arrived(arrival, from_pair)
    mine = half(core)
    total[...] += from_pair[...]
    base = Region(0, mine.rows, 0, mine.cols)
    bases = [base]
    for level, axes in enumerate(levels):
        slots = buffers[2 + level]
        steps = group_offsets(axes)
        stage, arrival = sems.stage(slots), sems.arrival()
        for slot, step in enumerate(steps):
            target = device_at(here, list(zip(axes, step)))
            sems.copy(shard_of(base, here, axes, step).at(total), slots.at[slot], target, stage, arrival)
        yield
        base = shard_of(base, here, axes, (0,) * len(axes))
        bases.append(base)
        sems.arrived(arrival, slots)
        result = base.load(total)
        for slot in range(len(steps)):
            result = result + slots[slot]
        if level + 1 < len(levels):
            base.store(total, result)
        else:
            base.moved(mine.row, mine.col).store(out, result * scale)
    for level in reversed(range(1, len(levels))):
        slots, axes = buffers[2 + level], levels[level]
        own = bases[level + 1].moved(mine.row, mine.col).at(out)
        stage, arrival = sems.stage(slots), sems.arrival()
        for step in group_offsets(axes):
            sems.copy(own, own, device_at(here, list(zip(axes, step))), stage, arrival)
        yield
        sems.arrived(arrival, slots)
    axes = levels[0]
    steps = group_offsets(axes)
    own = bases[1].moved(mine.row, mine.col).at(out)
    stage, arrivals = sems.stage(buffers[2]), [sems.arrival() for _ in steps]
    for step, arrival in zip(steps, arrivals):
        sems.copy(own, own, device_at(here, list(zip(axes, step))), stage, arrival)
    stage, last = sems.stage(from_pair), sems.arrival()
    sems.copy(own, own, far, stage, last)
    yield
    for step, arrival in reversed(list(zip(steps, arrivals))):
        back = tuple((RING - s) % RING for s in step)
        block = shard_of(bases[0], here, axes, back).moved(mine.row, mine.col).at(out)
        sems.arrived(arrival, block)
        sems.copy(block, block, far, stage, last)
    yield
    sems.arrived(last, from_pair)


def stages_of(levels):
    return 2 + 2 * len(levels)


def arrivals_of(levels):
    return stages_of(levels) - 1 + RING ** len(levels[0]) - 1


def tall(row, rows, apart):
    return lambda core: Region(row + core * apart, rows, 0, 256)


def wide(row, rows):
    return lambda core: Region(row, rows, core * 512, 512)


UNITS = (
    (DOWN2, tall(0, 512, 512), ORDERS[0]),
    (UP2, wide(0, 256), ORDERS[1]),
    (DOWN1, tall(0, 512, 512), ORDERS[2]),
    (UP1, wide(0, 256), ORDERS[0]),
    (IN, tall(0, 512, 1024), ORDERS[1]),
    (IN, tall(512, 512, 1024), ORDERS[2]),
)
PLAN = (
    "c0", "c1", "c2", "c3", "bar", "o0", "u0", "m0", "c4", "o1", "u1", "m1",
    "u0", "c5", "o2", "u2", "m2", "u1", "c6", "u2", "o3", "u3", "m3", "c7",
    "u3", "o4", "u4", "o5", "u5", "m4", "m5", "c8", "u4", "u5",
)


def tiles():
    return [pl.ds(at, TILE) for at in range(0, ROWS, TILE)]


def step_kernel(scale, *refs):
    inputs, refs = refs[:7], refs[7:]
    dx, *outs = refs[:6]
    refs = refs[6:]
    x, g, w_in, w_up1, w_down1, w_up2, w_down2 = refs[:7]
    refs = refs[7:]
    mid, act_one, slope_one, hid_two, act_three, slope_three, d_pre3, d_hid2, d_pre1, d_mid = refs[:10]
    refs = refs[10:]
    grads, refs = refs[: len(UNITS)], refs[len(UNITS) :]
    buffers, (loads, send, recv) = refs[:-3], refs[-3:]
    here = place()
    peers = greet(here, sorted({axes for _, _, levels in UNITS for axes in levels}))

    pending = {}
    number = 0
    for name, source, target in zip(("x", "g", "w_in", "w_up1", "w_down1", "w_up2", "w_down2"), inputs, refs_of(x, g, w_in, w_up1, w_down1, w_up2, w_down2)):
        pending[name] = []
        blocks = tiles() if name == "x" else [pl.ds(0, target.shape[0])]
        for block in blocks:
            pending[name].append(pltpu.make_async_copy(source.at[block], target.at[block], loads.at[number]))
            number += 1
    for name in ("w_in", "x", "w_up1", "w_down1", "w_up2", "g", "w_down2"):
        for copy in pending[name]:
            copy.start()

    def ready(name):
        for copy in pending.pop(name, []):
            copy.wait()

    def project():
        ready("w_in")
        for copy, rows in zip(pending.pop("x"), tiles()):
            copy.wait()
            mid[rows, :] = plain_product(x[rows, :], w_in[...]).astype(HALF)

    def expand(source, weight, name, act, slope):
        ready(name)
        for rows in tiles():
            value, rate = gelu_pair(plain_product(source[rows, :], weight[...]).astype(HALF))
            act[rows, :] = value.astype(HALF)
            slope[rows, :] = rate

    def second():
        ready("w_down1")
        for rows in tiles():
            hid_two[rows, :] = (plain_product(act_one[rows, :], w_down1[...]) + mid[rows, :].astype(WIDE)).astype(HALF)

    def before_gelu(source, weight, slope, target):
        for rows in tiles():
            grad = times_transposed(source[rows, :], weight[...]).astype(HALF)
            target[rows, :] = (grad.astype(WIDE) * slope[rows, :]).astype(HALF)

    def before_layer(source, weight, skip, target):
        for rows in tiles():
            target[rows, :] = (times_transposed(source[rows, :], weight[...]) + skip[rows, :].astype(WIDE)).astype(HALF)

    def third():
        expand(hid_two, w_up2, "w_up2", act_three, slope_three)
        ready("g")
        ready("w_down2")

    def leave():
        for rows in tiles():
            dx[rows, :] = times_transposed(d_mid[rows, :], w_in[...]).astype(HALF)

    stages = (
        project,
        lambda: expand(mid, w_up1, "w_up1", act_one, slope_one),
        second,
        third,
        lambda: before_gelu(g, w_down2, slope_three, d_pre3),
        lambda: before_layer(d_pre3, w_up2, g, d_hid2),
        lambda: before_gelu(d_hid2, w_down1, slope_one, d_pre1),
        lambda: before_layer(d_pre1, w_up1, d_hid2, d_mid),
        leave,
    )
    factors = {DOWN2: (act_three, g), UP2: (hid_two, d_pre3), DOWN1: (act_one, d_hid2), UP1: (mid, d_pre1), IN: (x, d_mid)}

    def gradient(unit, core):
        array, half, _ = UNITS[unit]
        first, other = factors[array]
        block = half(core)
        left = first[:, pl.ds(hinted(block.row, 128), block.rows)]
        right = other[:, pl.ds(hinted(block.col, 128), block.cols)]
        piece = rows_contract(left, right)
        if core is here["core"]:
            totals[unit][...] = piece
        else:
            grads[unit][...] = piece

    sems = Semaphores(send, recv)
    units, totals = [], []
    at = 0
    for array, half, levels in UNITS:
        count = len(buffer_shapes(half, levels))
        units.append(reduce_unit(here, levels, grads[len(units)], half, buffers[at : at + count], outs[array], sems, scale))
        totals.append(buffers[at + 1])
        at += count
    live = dict(enumerate(units))

    def advance(unit):
        if unit in live and next(live[unit], "done") == "done":
            del live[unit]

    for word in PLAN:
        if word == "bar":
            pl.semaphore_wait(pltpu.get_barrier_semaphore(), peers)
            continue
        kind, which = word[0], int(word[1:])
        if kind == "c":
            stages[which]()
        elif kind == "u":
            advance(which)
        else:
            gradient(which, 1 - here["core"] if kind == "o" else here["core"])
    for name in list(pending):
        ready(name)
    while live:
        for unit in list(live):
            advance(unit)
    sems.close()


def refs_of(*refs):
    return refs


def fused_step(args, scale):
    vmem = pltpu.VMEM
    inputs = ((ROWS, 2048), (ROWS, 256), (2048, 256), (256, 1024), (1024, 256), (256, 1024), (1024, 256))
    scratch = [vmem(shape, HALF) for shape in inputs]
    scratch += [
        vmem((ROWS, 256), HALF),
        vmem((ROWS, 1024), HALF),
        vmem((ROWS, 1024), WIDE),
        vmem((ROWS, 256), HALF),
        vmem((ROWS, 1024), HALF),
        vmem((ROWS, 1024), WIDE),
        vmem((ROWS, 1024), HALF),
        vmem((ROWS, 256), HALF),
        vmem((ROWS, 1024), HALF),
        vmem((ROWS, 256), HALF),
    ]
    scratch += [vmem(half(0).shape(), WIDE) for _, half, _ in UNITS]
    for _, half, levels in UNITS:
        scratch += [vmem(shape, WIDE) for shape in buffer_shapes(half, levels)]
    scratch += [pltpu.SemaphoreType.DMA((6 + ROWS // TILE,))]
    scratch += [pltpu.SemaphoreType.DMA((sum(count(levels) for _, _, levels in UNITS),)) for count in (stages_of, arrivals_of)]
    outs = [jax.ShapeDtypeStruct((ROWS, 2048), HALF)] + [jax.ShapeDtypeStruct(shape, WIDE) for shape in SHAPES]

    def body(*refs):
        step_kernel(scale, *refs)

    return pl.pallas_call(
        body,
        out_shape=outs,
        in_specs=[pl.BlockSpec(memory_space=pltpu.HBM)] * 7,
        out_specs=[pl.BlockSpec(memory_space=pltpu.VMEM)] * 6,
        scratch_shapes=scratch,
        compiler_params=pltpu.CompilerParams(collective_id=0, has_side_effects=True, vmem_limit_bytes=40 * 1024 * 1024),
    )(*args)


def deliver(arrays):
    count = len(arrays)

    def body(*refs):
        copies = [pltpu.make_async_copy(refs[i], refs[count + i], refs[-1].at[i]) for i in range(count)]
        for copy in copies:
            copy.start()
        for copy in copies:
            copy.wait()

    return pl.pallas_call(
        body,
        out_shape=[jax.ShapeDtypeStruct(array.shape, array.dtype) for array in arrays],
        in_specs=[pl.BlockSpec(memory_space=pl.ANY)] * count,
        out_specs=[pl.BlockSpec(memory_space=pl.ANY)] * count,
        scratch_shapes=[pltpu.SemaphoreType.DMA((count,))],
        compiler_params=pltpu.CompilerParams(vmem_limit_bytes=1024 * 1024),
    )(*arrays)


def solution(mesh):
    batch_axes = ("z", "y", "x")
    scale = 1.0 / math.prod(mesh.shape.values())
    row_spec = P(batch_axes, None)
    full_spec = P(None, None)

    def device_step(*args):
        args = [pltpu.with_memory_space_constraint(arg, pltpu.HBM) for arg in args]
        return tuple(deliver(fused_step(args, scale)))

    return jax.shard_map(
        device_step,
        mesh=mesh,
        in_specs=(row_spec, row_spec, full_spec, full_spec, full_spec, full_spec, full_spec),
        out_specs=(row_spec, full_spec, full_spec, full_spec, full_spec, full_spec),
        check_vma=False,
    )
```

```python
import itertools
import math
import jax
import jax.numpy as jnp
from jax import lax
from jax.experimental import pallas as pl
from jax.experimental.pallas import tpu as pltpu
from jax.sharding import PartitionSpec as P

SQRT_HALF = 0.7071067811865476
INV_SQRT_TAU = 0.3989422804014327
MESH = pl.DeviceIdType.MESH
RING = 4
ROWS = 1024
TILE = 512
HALF, WIDE = jnp.bfloat16, jnp.float32
IN, UP1, DOWN1, UP2, DOWN2 = range(5)
SHAPES = ((2048, 256), (256, 1024), (1024, 256), (256, 1024), (1024, 256))
ORDERS = ((("x",), ("y", "z")), (("y",), ("z", "x")), (("z",), ("x", "y")))


def gelu_pair(pre_act):
    wide = pre_act.astype(WIDE)
    share = 0.5 * (1.0 + lax.erf(wide * SQRT_HALF))
    return wide * share, share + wide * jnp.exp(-0.5 * wide * wide) * INV_SQRT_TAU


def plain_product(first_op, second_op):
    return lax.dot_general(first_op, second_op, (((1,), (0,)), ((), ())), preferred_element_type=jnp.float32)


def rows_contract(first_op, second_op):
    return lax.dot_general(first_op, second_op, (((0,), (0,)), ((), ())), preferred_element_type=jnp.float32)


def times_transposed(first_op, second_op):
    return lax.dot_general(first_op, second_op, (((1,), (1,)), ((), ())), preferred_element_type=jnp.float32)


def hinted(value, step):
    return value if isinstance(value, int) else pl.multiple_of(value, step)


class Region:
    def __init__(self, row, rows, col, cols):
        self.row, self.rows, self.col, self.cols = row, rows, col, cols

    def at(self, ref):
        return ref.at[pl.ds(hinted(self.row, 8), self.rows), pl.ds(hinted(self.col, 128), self.cols)]

    def load(self, ref):
        return ref[pl.ds(hinted(self.row, 8), self.rows), pl.ds(hinted(self.col, 128), self.cols)]

    def store(self, ref, value):
        ref[pl.ds(hinted(self.row, 8), self.rows), pl.ds(hinted(self.col, 128), self.cols)] = value

    def part(self, index, count):
        if self.rows // count >= 8:
            step = self.rows // count
            return Region(self.row + index * step, step, self.col, self.cols)
        step = self.cols // count
        if step >= 128:
            return Region(self.row, self.rows, self.col + index * step, step)
        rows, cols = self.rows // 2, self.cols // (count // 2)
        across = self.cols // cols
        return Region(self.row + index // across * rows, rows, self.col + lax.rem(index, across) * cols, cols)

    def shape(self):
        return (self.rows, self.cols)

    def moved(self, row, col):
        return Region(self.row + row, self.rows, self.col + col, self.cols)


class Semaphores:
    def __init__(self, send, recv):
        self.send, self.recv, self.sends, self.recvs, self.closing = send, recv, 0, 0, []

    def stage(self, span):
        number = self.sends
        self.sends += 1
        self.closing.append((number, span))
        return number

    def arrival(self):
        self.recvs += 1
        return self.recvs - 1

    def copy(self, source, target, device, stage, arrival):
        pltpu.make_async_remote_copy(
            src_ref=source,
            dst_ref=target,
            send_sem=self.send.at[stage],
            recv_sem=self.recv.at[arrival],
            device_id=device,
            device_id_type=MESH,
        ).start()

    def arrived(self, arrival, span):
        pltpu.make_async_copy(span, span, self.recv.at[arrival]).wait()

    def close(self):
        for number, span in self.closing:
            pltpu.make_async_copy(span, span, self.send.at[number]).wait()


def place():
    x = lax.axis_index("x")
    return {"x": x // 2, "y": lax.axis_index("y"), "z": lax.axis_index("z"), "core": lax.rem(x, 2)}


def device_at(here, offsets):
    where = {}
    for axis, step in offsets:
        other = lax.rem(here[axis] + step, RING)
        where[axis] = other * 2 + here["core"] if axis == "x" else other
    return where


def partner(here):
    return {"x": here["x"] * 2 + 1 - here["core"]}


def group_offsets(axes):
    steps = list(itertools.product(range(RING), repeat=len(axes)))[1:]
    steps.sort(key=lambda step: -sum(min(s, RING - s) for s in step))
    return steps


def greet(here, groups):
    barrier = pltpu.get_barrier_semaphore()
    peers = {(("core", 1),): partner(here)}
    for axes in groups:
        for step in group_offsets(axes):
            key = tuple(sorted((axis, s) for axis, s in zip(axes, step) if s))
            peers[key] = device_at(here, key)
    for peer in peers.values():
        pl.semaphore_signal(barrier, inc=1, device_id=peer, device_id_type=MESH)
    return len(peers)


def shard_of(block, here, axes, step):
    for axis, s in zip(axes, step):
        block = block.part(lax.rem(here[axis] + s, RING) if s else here[axis], RING)
    return block


def buffer_shapes(half, levels):
    block = half(0)
    shapes = [block.shape(), block.shape()]
    for axes in levels:
        for _ in axes:
            block = block.part(0, RING)
        shapes.append((RING ** len(axes) - 1,) + block.shape())
    return shapes


def reduce_unit(here, levels, grad, half, buffers, out, sems, scale):
    core = here["core"]
    far = partner(here)
    from_pair, total = buffers[0], buffers[1]
    arrival = sems.arrival()
    sems.copy(grad, from_pair, far, sems.stage(from_pair), arrival)
    yield
    sems.arrived(arrival, from_pair)
    mine = half(core)
    total[...] += from_pair[...]
    base = Region(0, mine.rows, 0, mine.cols)
    bases = [base]
    for level, axes in enumerate(levels):
        slots = buffers[2 + level]
        steps = group_offsets(axes)
        stage, arrival = sems.stage(slots), sems.arrival()
        for slot, step in enumerate(steps):
            target = device_at(here, list(zip(axes, step)))
            sems.copy(shard_of(base, here, axes, step).at(total), slots.at[slot], target, stage, arrival)
        yield
        base = shard_of(base, here, axes, (0,) * len(axes))
        bases.append(base)
        sems.arrived(arrival, slots)
        result = base.load(total)
        for slot in range(len(steps)):
            result = result + slots[slot]
        if level + 1 < len(levels):
            base.store(total, result)
        else:
            base.moved(mine.row, mine.col).store(out, result * scale)
    for level in reversed(range(1, len(levels))):
        slots, axes = buffers[2 + level], levels[level]
        own = bases[level + 1].moved(mine.row, mine.col).at(out)
        stage, arrival = sems.stage(slots), sems.arrival()
        for step in group_offsets(axes):
            sems.copy(own, own, device_at(here, list(zip(axes, step))), stage, arrival)
        yield
        sems.arrived(arrival, slots)
    axes = levels[0]
    steps = group_offsets(axes)
    own = bases[1].moved(mine.row, mine.col).at(out)
    stage, arrivals = sems.stage(buffers[2]), [sems.arrival() for _ in steps]
    for step, arrival in zip(steps, arrivals):
        sems.copy(own, own, device_at(here, list(zip(axes, step))), stage, arrival)
    stage, last = sems.stage(from_pair), sems.arrival()
    sems.copy(own, own, far, stage, last)
    yield
    for step, arrival in reversed(list(zip(steps, arrivals))):
        back = tuple((RING - s) % RING for s in step)
        block = shard_of(bases[0], here, axes, back).moved(mine.row, mine.col).at(out)
        sems.arrived(arrival, block)
        sems.copy(block, block, far, stage, last)
    yield
    sems.arrived(last, from_pair)


def stages_of(levels):
    return 2 + 2 * len(levels)


def arrivals_of(levels):
    return stages_of(levels) - 1 + RING ** len(levels[0]) - 1


def tall(row, rows, apart):
    return lambda core: Region(row + core * apart, rows, 0, 256)


def wide(row, rows):
    return lambda core: Region(row, rows, core * 512, 512)


UNITS = (
    (DOWN2, tall(0, 512, 512), ORDERS[0]),
    (UP2, wide(0, 256), ORDERS[1]),
    (DOWN1, tall(0, 512, 512), ORDERS[2]),
    (UP1, wide(0, 128), ORDERS[1]),
    (UP1, wide(128, 128), ORDERS[2]),
    (IN, tall(0, 512, 1024), ORDERS[0]),
    (IN, tall(512, 256, 1024), ORDERS[1]),
    (IN, tall(768, 256, 1024), ORDERS[2]),
)

PLAN = (
    "c0", "c1", "c2", "c3", "bar", "o0", "u0", "m0", "c4", "o1", "u1", "m1",
    "u0", "c5", "o2", "u2", "m2", "u1", "c6", "u2", "o3", "u3", "o4", "u4",
    "m3", "m4", "c7", "u3", "u4", "o5", "u5", "o6", "u6", "o7", "u7", "m5",
    "m6", "m7", "c8", "u5", "u6", "u7",
)


def tiles():
    return [pl.ds(at, TILE) for at in range(0, ROWS, TILE)]


def step_kernel(scale, *refs):
    inputs, refs = refs[:7], refs[7:]
    dx, *outs = refs[:6]
    refs = refs[6:]
    x, g, w_in, w_up1, w_down1, w_up2, w_down2 = refs[:7]
    refs = refs[7:]
    mid, act_one, slope_one, hid_two, act_three, slope_three, d_pre3, d_hid2, d_pre1, d_mid = refs[:10]
    refs = refs[10:]
    grads, refs = refs[: len(UNITS)], refs[len(UNITS) :]
    buffers, (loads, send, recv) = refs[:-3], refs[-3:]
    here = place()
    peers = greet(here, sorted({axes for _, _, levels in UNITS for axes in levels}))

    core = here["core"]
    order = (1 - core, core)
    number = 0
    pending = []
    for source, target, axis in zip(inputs, refs_of(x, g, w_in, w_up1, w_down1, w_up2, w_down2), (1, None, 0, 1, 0, 1, 0)):
        size = target.shape[axis or 0] // (1 if axis is None else 2)
        for place_here, place_there in enumerate((0,) if axis is None else order):
            there, to = pl.ds(hinted(place_there * size, size), size), pl.ds(place_here * size, size)
            where = (there, to) if axis != 1 else ((slice(None), there), (slice(None), to))
            pending.append(pltpu.make_async_copy(source.at[where[0]], target.at[where[1]], loads.at[number]))
            number += 1
    for copy in pending:
        copy.start()

    def project():
        for copy in pending:
            copy.wait()
        for rows in tiles():
            mid[rows, :] = plain_product(x[rows, :], w_in[...]).astype(HALF)

    def expand(source, weight, act, slope):
        for rows in tiles():
            value, rate = gelu_pair(plain_product(source[rows, :], weight[...]).astype(HALF))
            act[rows, :] = value.astype(HALF)
            slope[rows, :] = rate

    def second():
        for rows in tiles():
            hid_two[rows, :] = (plain_product(act_one[rows, :], w_down1[...]) + mid[rows, :].astype(WIDE)).astype(HALF)

    def before_gelu(source, weight, slope, target):
        for rows in tiles():
            grad = times_transposed(source[rows, :], weight[...]).astype(HALF)
            target[rows, :] = (grad.astype(WIDE) * slope[rows, :]).astype(HALF)

    def before_layer(source, weight, skip, target):
        for rows in tiles():
            target[rows, :] = (times_transposed(source[rows, :], weight[...]) + skip[rows, :].astype(WIDE)).astype(HALF)

    def third():
        expand(hid_two, w_up2, act_three, slope_three)

    def leave():
        for place_here, place_there in enumerate(order):
            columns = pl.ds(hinted(place_there * 1024, 1024), 1024)
            for rows in tiles():
                dx[rows, columns] = times_transposed(d_mid[rows, :], w_in[pl.ds(place_here * 1024, 1024), :]).astype(HALF)

    stages = (
        project,
        lambda: expand(mid, w_up1, act_one, slope_one),
        second,
        third,
        lambda: before_gelu(g, w_down2, slope_three, d_pre3),
        lambda: before_layer(d_pre3, w_up2, g, d_hid2),
        lambda: before_gelu(d_hid2, w_down1, slope_one, d_pre1),
        lambda: before_layer(d_pre1, w_up1, d_hid2, d_mid),
        leave,
    )
    factors = {DOWN2: (act_three, g), UP2: (hid_two, d_pre3), DOWN1: (act_one, d_hid2), UP1: (mid, d_pre1), IN: (x, d_mid)}

    def gradient(unit, own):
        array, half, _ = UNITS[unit]
        first, other = factors[array]
        block = half(own)
        left = first[:, block.row : block.row + block.rows]
        right = other[:, block.col : block.col + block.cols]
        (totals if own else grads)[unit][...] = rows_contract(left, right)

    sems = Semaphores(send, recv)
    units, totals = [], []
    at = 0
    for array, half, levels in UNITS:
        count = len(buffer_shapes(half, levels))
        units.append(reduce_unit(here, levels, grads[len(units)], half, buffers[at : at + count], outs[array], sems, scale))
        totals.append(buffers[at + 1])
        at += count
    live = dict(enumerate(units))

    def advance(unit):
        if unit in live and next(live[unit], "done") == "done":
            del live[unit]

    for word in PLAN:
        if word == "bar":
            pl.semaphore_wait(pltpu.get_barrier_semaphore(), peers)
            continue
        kind, which = word[0], int(word[1:])
        if kind == "c":
            stages[which]()
        elif kind == "u":
            advance(which)
        else:
            gradient(which, 0 if kind == "o" else 1)
    while live:
        for unit in list(live):
            advance(unit)
    sems.close()


def refs_of(*refs):
    return refs


def fused_step(args, scale):
    vmem = pltpu.VMEM
    inputs = ((ROWS, 2048), (ROWS, 256), (2048, 256), (256, 1024), (1024, 256), (256, 1024), (1024, 256))
    scratch = [vmem(shape, HALF) for shape in inputs]
    scratch += [
        vmem((ROWS, 256), HALF),
        vmem((ROWS, 1024), HALF),
        vmem((ROWS, 1024), WIDE),
        vmem((ROWS, 256), HALF),
        vmem((ROWS, 1024), HALF),
        vmem((ROWS, 1024), WIDE),
        vmem((ROWS, 1024), HALF),
        vmem((ROWS, 256), HALF),
        vmem((ROWS, 1024), HALF),
        vmem((ROWS, 256), HALF),
    ]
    scratch += [vmem(half(0).shape(), WIDE) for _, half, _ in UNITS]
    for _, half, levels in UNITS:
        scratch += [vmem(shape, WIDE) for shape in buffer_shapes(half, levels)]
    scratch += [pltpu.SemaphoreType.DMA((13,))]
    scratch += [pltpu.SemaphoreType.DMA((sum(count(levels) for _, _, levels in UNITS),)) for count in (stages_of, arrivals_of)]
    outs = [jax.ShapeDtypeStruct((ROWS, 2048), HALF)] + [jax.ShapeDtypeStruct(shape, WIDE) for shape in SHAPES]

    def body(*refs):
        step_kernel(scale, *refs)

    return pl.pallas_call(
        body,
        out_shape=outs,
        in_specs=[pl.BlockSpec(memory_space=pltpu.HBM)] * 7,
        out_specs=[pl.BlockSpec(memory_space=pltpu.VMEM)] * 6,
        scratch_shapes=scratch,
        compiler_params=pltpu.CompilerParams(collective_id=0, has_side_effects=True, vmem_limit_bytes=40 * 1024 * 1024),
    )(*args)


def deliver(arrays):
    count = len(arrays)

    def body(*refs):
        copies = [pltpu.make_async_copy(refs[i], refs[count + i], refs[-1].at[i]) for i in range(count)]
        for copy in copies:
            copy.start()
        for copy in copies:
            copy.wait()

    return pl.pallas_call(
        body,
        out_shape=[jax.ShapeDtypeStruct(array.shape, array.dtype) for array in arrays],
        in_specs=[pl.BlockSpec(memory_space=pl.ANY)] * count,
        out_specs=[pl.BlockSpec(memory_space=pl.ANY)] * count,
        scratch_shapes=[pltpu.SemaphoreType.DMA((count,))],
        compiler_params=pltpu.CompilerParams(vmem_limit_bytes=1024 * 1024),
    )(*arrays)


def solution(mesh):
    batch_axes = ("z", "y", "x")
    scale = 1.0 / math.prod(mesh.shape.values())
    row_spec = P(batch_axes, None)
    full_spec = P(None, None)

    def device_step(*args):
        args = [pltpu.with_memory_space_constraint(arg, pltpu.HBM) for arg in args]
        return tuple(deliver(fused_step(args, scale)))

    return jax.shard_map(
        device_step,
        mesh=mesh,
        in_specs=(row_spec, row_spec, full_spec, full_spec, full_spec, full_spec, full_spec),
        out_specs=(row_spec, full_spec, full_spec, full_spec, full_spec, full_spec),
        check_vma=False,
    )
```

```python
import itertools
import math
import jax
import jax.numpy as jnp
from jax import lax
from jax.experimental import pallas as pl
from jax.experimental.pallas import tpu as pltpu
from jax.sharding import PartitionSpec as P

SQRT_HALF = 0.7071067811865476
INV_SQRT_TAU = 0.3989422804014327
MESH = pl.DeviceIdType.MESH
RING = 4
ROWS = 1024
TILE = 512
HALF, WIDE = jnp.bfloat16, jnp.float32
IN, UP1, DOWN1, UP2, DOWN2 = range(5)
SHAPES = ((2048, 256), (256, 1024), (1024, 256), (256, 1024), (1024, 256))
ORDERS = ((("x",), ("y", "z")), (("y",), ("z", "x")), (("z",), ("x", "y")))


def gelu_pair(pre_act):
    wide = pre_act.astype(WIDE)
    share = 0.5 * (1.0 + lax.erf(wide * SQRT_HALF))
    return wide * share, share + wide * jnp.exp(-0.5 * wide * wide) * INV_SQRT_TAU


def plain_product(first_op, second_op):
    return lax.dot_general(first_op, second_op, (((1,), (0,)), ((), ())), preferred_element_type=jnp.float32)


def rows_contract(first_op, second_op):
    return lax.dot_general(first_op, second_op, (((0,), (0,)), ((), ())), preferred_element_type=jnp.float32)


def times_transposed(first_op, second_op):
    return lax.dot_general(first_op, second_op, (((1,), (1,)), ((), ())), preferred_element_type=jnp.float32)


def hinted(value, step):
    return value if isinstance(value, int) else pl.multiple_of(value, step)


class Region:
    def __init__(self, row, rows, col, cols):
        self.row, self.rows, self.col, self.cols = row, rows, col, cols

    def at(self, ref):
        return ref.at[pl.ds(hinted(self.row, 8), self.rows), pl.ds(hinted(self.col, 128), self.cols)]

    def load(self, ref):
        return ref[pl.ds(hinted(self.row, 8), self.rows), pl.ds(hinted(self.col, 128), self.cols)]

    def store(self, ref, value):
        ref[pl.ds(hinted(self.row, 8), self.rows), pl.ds(hinted(self.col, 128), self.cols)] = value

    def part(self, index, count):
        if self.rows // count >= 8:
            step = self.rows // count
            return Region(self.row + index * step, step, self.col, self.cols)
        step = self.cols // count
        if step >= 128:
            return Region(self.row, self.rows, self.col + index * step, step)
        rows, cols = self.rows // 2, self.cols // (count // 2)
        across = self.cols // cols
        return Region(self.row + index // across * rows, rows, self.col + lax.rem(index, across) * cols, cols)

    def shape(self):
        return (self.rows, self.cols)

    def moved(self, row, col):
        return Region(self.row + row, self.rows, self.col + col, self.cols)


class Semaphores:
    def __init__(self, send, recv):
        self.send, self.recv, self.sends, self.recvs, self.closing = send, recv, 0, 0, []

    def stage(self, span):
        number = self.sends
        self.sends += 1
        self.closing.append((number, span))
        return number

    def arrival(self):
        self.recvs += 1
        return self.recvs - 1

    def copy(self, source, target, device, stage, arrival):
        pltpu.make_async_remote_copy(
            src_ref=source,
            dst_ref=target,
            send_sem=self.send.at[stage],
            recv_sem=self.recv.at[arrival],
            device_id=device,
            device_id_type=MESH,
        ).start()

    def arrived(self, arrival, span):
        pltpu.make_async_copy(span, span, self.recv.at[arrival]).wait()

    def close(self):
        for number, span in self.closing:
            pltpu.make_async_copy(span, span, self.send.at[number]).wait()


def place():
    x = lax.axis_index("x")
    return {"x": x // 2, "y": lax.axis_index("y"), "z": lax.axis_index("z"), "core": lax.rem(x, 2)}


def device_at(here, offsets):
    where = {}
    for axis, step in offsets:
        other = lax.rem(here[axis] + step, RING)
        where[axis] = other * 2 + here["core"] if axis == "x" else other
    return where


def partner(here):
    return {"x": here["x"] * 2 + 1 - here["core"]}


def group_offsets(axes):
    steps = list(itertools.product(range(RING), repeat=len(axes)))[1:]
    steps.sort(key=lambda step: -sum(min(s, RING - s) for s in step))
    return steps


def greet(here, groups):
    barrier = pltpu.get_barrier_semaphore()
    peers = {(("core", 1),): partner(here)}
    for axes in groups:
        for step in group_offsets(axes):
            key = tuple(sorted((axis, s) for axis, s in zip(axes, step) if s))
            peers[key] = device_at(here, key)
    for peer in peers.values():
        pl.semaphore_signal(barrier, inc=1, device_id=peer, device_id_type=MESH)
    return len(peers)


def shard_of(block, here, axes, step):
    for axis, s in zip(axes, step):
        block = block.part(lax.rem(here[axis] + s, RING) if s else here[axis], RING)
    return block


def buffer_shapes(half, levels):
    block = half(0)
    shapes = [block.shape(), block.shape()]
    for axes in levels:
        for _ in axes:
            block = block.part(0, RING)
        shapes.append((RING ** len(axes) - 1,) + block.shape())
    return shapes


def reduce_unit(here, levels, grad, half, buffers, out, sems, scale):
    core = here["core"]
    far = partner(here)
    from_pair, total = buffers[0], buffers[1]
    arrival = sems.arrival()
    sems.copy(grad, from_pair, far, sems.stage(from_pair), arrival)
    yield
    sems.arrived(arrival, from_pair)
    mine = half(core)
    total[...] += from_pair[...]
    base = Region(0, mine.rows, 0, mine.cols)
    bases = [base]
    for level, axes in enumerate(levels):
        slots = buffers[2 + level]
        steps = group_offsets(axes)
        stage, arrival = sems.stage(slots), sems.arrival()
        for slot, step in enumerate(steps):
            target = device_at(here, list(zip(axes, step)))
            sems.copy(shard_of(base, here, axes, step).at(total), slots.at[slot], target, stage, arrival)
        yield
        base = shard_of(base, here, axes, (0,) * len(axes))
        bases.append(base)
        sems.arrived(arrival, slots)
        result = base.load(total)
        for slot in range(len(steps)):
            result = result + slots[slot]
        if level + 1 < len(levels):
            base.store(total, result)
        else:
            base.moved(mine.row, mine.col).store(out, result * scale)
    for level in reversed(range(1, len(levels))):
        slots, axes = buffers[2 + level], levels[level]
        own = bases[level + 1].moved(mine.row, mine.col).at(out)
        stage, arrival = sems.stage(slots), sems.arrival()
        for step in group_offsets(axes):
            sems.copy(own, own, device_at(here, list(zip(axes, step))), stage, arrival)
        yield
        sems.arrived(arrival, slots)
    axes = levels[0]
    steps = group_offsets(axes)
    own = bases[1].moved(mine.row, mine.col).at(out)
    stage, arrivals = sems.stage(buffers[2]), [sems.arrival() for _ in steps]
    for step, arrival in zip(steps, arrivals):
        sems.copy(own, own, device_at(here, list(zip(axes, step))), stage, arrival)
    stage, last = sems.stage(from_pair), sems.arrival()
    sems.copy(own, own, far, stage, last)
    yield
    for step, arrival in reversed(list(zip(steps, arrivals))):
        back = tuple((RING - s) % RING for s in step)
        block = shard_of(bases[0], here, axes, back).moved(mine.row, mine.col).at(out)
        sems.arrived(arrival, block)
        sems.copy(block, block, far, stage, last)
    yield
    sems.arrived(last, from_pair)


def stages_of(levels):
    return 2 + 2 * len(levels)


def arrivals_of(levels):
    return stages_of(levels) - 1 + RING ** len(levels[0]) - 1


def tall(row, rows, apart):
    return lambda core: Region(row + core * apart, rows, 0, 256)


def wide(row, rows):
    return lambda core: Region(row, rows, core * 512, 512)


UNITS = (
    (DOWN2, tall(0, 512, 512), ORDERS[0]),
    (UP2, wide(0, 256), ORDERS[1]),
    (DOWN1, tall(0, 512, 512), ORDERS[2]),
    (UP1, wide(0, 128), ORDERS[1]),
    (UP1, wide(128, 128), ORDERS[2]),
    (IN, tall(0, 512, 1024), ORDERS[0]),
    (IN, tall(512, 256, 1024), ORDERS[1]),
    (IN, tall(768, 256, 1024), ORDERS[2]),
)

PLAN = (
    "c0", "c1", "c2", "c3", "bar", "o0", "u0", "m0", "c4", "o1", "u1", "m1",
    "c5", "u0", "o2", "u2", "m2", "c6", "u1", "o3", "u3", "o4", "u4", "m3",
    "m4", "u2", "c7", "o5", "u5", "o6", "u6", "o7", "u7", "u3", "u4", "m5",
    "m6", "m7", "c8", "u5", "u6", "u7",
)


def tiles():
    return [pl.ds(at, TILE) for at in range(0, ROWS, TILE)]


def step_kernel(scale, *refs):
    inputs, refs = refs[:7], refs[7:]
    dx, *outs = refs[:6]
    refs = refs[6:]
    x, g, w_in, w_up1, w_down1, w_up2, w_down2 = refs[:7]
    refs = refs[7:]
    mid, act_one, slope_one, hid_two, act_three, slope_three, d_pre3, d_hid2, d_pre1, d_mid = refs[:10]
    refs = refs[10:]
    grads, refs = refs[: len(UNITS)], refs[len(UNITS) :]
    buffers, (loads, send, recv) = refs[:-3], refs[-3:]
    here = place()
    peers = greet(here, sorted({axes for _, _, levels in UNITS for axes in levels}))

    core = here["core"]
    order = (1 - core, core)
    number = 0
    pending = []
    for source, target, axis in zip(inputs, refs_of(x, g, w_in, w_up1, w_down1, w_up2, w_down2), (1, None, 0, 1, 0, 1, 0)):
        size = target.shape[axis or 0] // (1 if axis is None else 2)
        for place_here, place_there in enumerate((0,) if axis is None else order):
            there, to = pl.ds(hinted(place_there * size, size), size), pl.ds(place_here * size, size)
            where = (there, to) if axis != 1 else ((slice(None), there), (slice(None), to))
            pending.append(pltpu.make_async_copy(source.at[where[0]], target.at[where[1]], loads.at[number]))
            number += 1
    for copy in pending:
        copy.start()

    def project():
        for copy in pending:
            copy.wait()
        for rows in tiles():
            mid[rows, :] = plain_product(x[rows, :], w_in[...]).astype(HALF)

    def expand(source, weight, act, slope):
        for rows in tiles():
            value, rate = gelu_pair(plain_product(source[rows, :], weight[...]).astype(HALF))
            act[rows, :] = value.astype(HALF)
            slope[rows, :] = rate

    def second():
        for rows in tiles():
            hid_two[rows, :] = (plain_product(act_one[rows, :], w_down1[...]) + mid[rows, :].astype(WIDE)).astype(HALF)

    def before_gelu(source, weight, slope, target):
        for rows in tiles():
            grad = times_transposed(source[rows, :], weight[...]).astype(HALF)
            target[rows, :] = (grad.astype(WIDE) * slope[rows, :]).astype(HALF)

    def before_layer(source, weight, skip, target):
        for rows in tiles():
            target[rows, :] = (times_transposed(source[rows, :], weight[...]) + skip[rows, :].astype(WIDE)).astype(HALF)

    def third():
        expand(hid_two, w_up2, act_three, slope_three)

    def leave():
        for place_here, place_there in enumerate(order):
            columns = pl.ds(hinted(place_there * 1024, 1024), 1024)
            for rows in tiles():
                dx[rows, columns] = times_transposed(d_mid[rows, :], w_in[pl.ds(place_here * 1024, 1024), :]).astype(HALF)

    stages = (
        project,
        lambda: expand(mid, w_up1, act_one, slope_one),
        second,
        third,
        lambda: before_gelu(g, w_down2, slope_three, d_pre3),
        lambda: before_layer(d_pre3, w_up2, g, d_hid2),
        lambda: before_gelu(d_hid2, w_down1, slope_one, d_pre1),
        lambda: before_layer(d_pre1, w_up1, d_hid2, d_mid),
        leave,
    )
    factors = {DOWN2: (act_three, g), UP2: (hid_two, d_pre3), DOWN1: (act_one, d_hid2), UP1: (mid, d_pre1), IN: (x, d_mid)}

    def gradient(unit, own):
        array, half, _ = UNITS[unit]
        first, other = factors[array]
        block = half(own)
        left = first[:, block.row : block.row + block.rows]
        right = other[:, block.col : block.col + block.cols]
        (totals if own else grads)[unit][...] = rows_contract(left, right)

    sems = Semaphores(send, recv)
    units, totals = [], []
    at = 0
    for array, half, levels in UNITS:
        count = len(buffer_shapes(half, levels))
        units.append(reduce_unit(here, levels, grads[len(units)], half, buffers[at : at + count], outs[array], sems, scale))
        totals.append(buffers[at + 1])
        at += count
    live = dict(enumerate(units))

    def advance(unit):
        if unit in live and next(live[unit], "done") == "done":
            del live[unit]

    for word in PLAN:
        if word == "bar":
            pl.semaphore_wait(pltpu.get_barrier_semaphore(), peers)
            continue
        kind, which = word[0], int(word[1:])
        if kind == "c":
            stages[which]()
        elif kind == "u":
            advance(which)
        else:
            gradient(which, 0 if kind == "o" else 1)
    while live:
        for unit in list(live):
            advance(unit)
    sems.close()


def refs_of(*refs):
    return refs


def fused_step(args, scale):
    vmem = pltpu.VMEM
    inputs = ((ROWS, 2048), (ROWS, 256), (2048, 256), (256, 1024), (1024, 256), (256, 1024), (1024, 256))
    scratch = [vmem(shape, HALF) for shape in inputs]
    scratch += [
        vmem((ROWS, 256), HALF),
        vmem((ROWS, 1024), HALF),
        vmem((ROWS, 1024), WIDE),
        vmem((ROWS, 256), HALF),
        vmem((ROWS, 1024), HALF),
        vmem((ROWS, 1024), WIDE),
        vmem((ROWS, 1024), HALF),
        vmem((ROWS, 256), HALF),
        vmem((ROWS, 1024), HALF),
        vmem((ROWS, 256), HALF),
    ]
    scratch += [vmem(half(0).shape(), WIDE) for _, half, _ in UNITS]
    for _, half, levels in UNITS:
        scratch += [vmem(shape, WIDE) for shape in buffer_shapes(half, levels)]
    scratch += [pltpu.SemaphoreType.DMA((13,))]
    scratch += [pltpu.SemaphoreType.DMA((sum(count(levels) for _, _, levels in UNITS),)) for count in (stages_of, arrivals_of)]
    outs = [jax.ShapeDtypeStruct((ROWS, 2048), HALF)] + [jax.ShapeDtypeStruct(shape, WIDE) for shape in SHAPES]

    def body(*refs):
        step_kernel(scale, *refs)

    return pl.pallas_call(
        body,
        out_shape=outs,
        in_specs=[pl.BlockSpec(memory_space=pltpu.HBM)] * 7,
        out_specs=[pl.BlockSpec(memory_space=pltpu.VMEM)] * 6,
        scratch_shapes=scratch,
        compiler_params=pltpu.CompilerParams(collective_id=0, has_side_effects=True, vmem_limit_bytes=40 * 1024 * 1024),
    )(*args)


def deliver(arrays):
    count = len(arrays)

    def body(*refs):
        copies = [pltpu.make_async_copy(refs[i], refs[count + i], refs[-1].at[i]) for i in range(count)]
        for copy in copies:
            copy.start()
        for copy in copies:
            copy.wait()

    return pl.pallas_call(
        body,
        out_shape=[jax.ShapeDtypeStruct(array.shape, array.dtype) for array in arrays],
        in_specs=[pl.BlockSpec(memory_space=pl.ANY)] * count,
        out_specs=[pl.BlockSpec(memory_space=pl.ANY)] * count,
        scratch_shapes=[pltpu.SemaphoreType.DMA((count,))],
        compiler_params=pltpu.CompilerParams(vmem_limit_bytes=1024 * 1024),
    )(*arrays)


def solution(mesh):
    batch_axes = ("z", "y", "x")
    scale = 1.0 / math.prod(mesh.shape.values())
    row_spec = P(batch_axes, None)
    full_spec = P(None, None)

    def device_step(*args):
        args = [pltpu.with_memory_space_constraint(arg, pltpu.HBM) for arg in args]
        return tuple(deliver(fused_step(args, scale)))

    return jax.shard_map(
        device_step,
        mesh=mesh,
        in_specs=(row_spec, row_spec, full_spec, full_spec, full_spec, full_spec, full_spec),
        out_specs=(row_spec, full_spec, full_spec, full_spec, full_spec, full_spec),
        check_vma=False,
    )
```

```python
import itertools
import math
import jax
import jax.numpy as jnp
from jax import lax
from jax.experimental import pallas as pl
from jax.experimental.pallas import tpu as pltpu
from jax.sharding import PartitionSpec as P

SQRT_HALF = 0.7071067811865476
INV_SQRT_TAU = 0.3989422804014327
MESH = pl.DeviceIdType.MESH
RING = 4
ROWS = 1024
TILE = 512
HALF, WIDE = jnp.bfloat16, jnp.float32
IN, UP1, DOWN1, UP2, DOWN2 = range(5)
SHAPES = ((2048, 256), (256, 1024), (1024, 256), (256, 1024), (1024, 256))
ORDERS = ((("x",), ("y", "z")), (("y",), ("z", "x")), (("z",), ("x", "y")))


def gelu_pair(pre_act):
    wide = pre_act.astype(WIDE)
    share = 0.5 * (1.0 + lax.erf(wide * SQRT_HALF))
    return wide * share, share + wide * jnp.exp(-0.5 * wide * wide) * INV_SQRT_TAU


def plain_product(first_op, second_op):
    return lax.dot_general(first_op, second_op, (((1,), (0,)), ((), ())), preferred_element_type=jnp.float32)


def rows_contract(first_op, second_op):
    return lax.dot_general(first_op, second_op, (((0,), (0,)), ((), ())), preferred_element_type=jnp.float32)


def times_transposed(first_op, second_op):
    return lax.dot_general(first_op, second_op, (((1,), (1,)), ((), ())), preferred_element_type=jnp.float32)


def hinted(value, step):
    return value if isinstance(value, int) else pl.multiple_of(value, step)


class Region:
    def __init__(self, row, rows, col, cols):
        self.row, self.rows, self.col, self.cols = row, rows, col, cols

    def at(self, ref):
        return ref.at[pl.ds(hinted(self.row, 8), self.rows), pl.ds(hinted(self.col, 128), self.cols)]

    def load(self, ref):
        return ref[pl.ds(hinted(self.row, 8), self.rows), pl.ds(hinted(self.col, 128), self.cols)]

    def store(self, ref, value):
        ref[pl.ds(hinted(self.row, 8), self.rows), pl.ds(hinted(self.col, 128), self.cols)] = value

    def part(self, index, count):
        if self.rows // count >= 8:
            step = self.rows // count
            return Region(self.row + index * step, step, self.col, self.cols)
        step = self.cols // count
        if step >= 128:
            return Region(self.row, self.rows, self.col + index * step, step)
        rows, cols = self.rows // 2, self.cols // (count // 2)
        across = self.cols // cols
        return Region(self.row + index // across * rows, rows, self.col + lax.rem(index, across) * cols, cols)

    def shape(self):
        return (self.rows, self.cols)

    def moved(self, row, col):
        return Region(self.row + row, self.rows, self.col + col, self.cols)


class Semaphores:
    def __init__(self, send, recv):
        self.send, self.recv, self.sends, self.recvs, self.closing = send, recv, 0, 0, []

    def stage(self, span):
        number = self.sends
        self.sends += 1
        self.closing.append((number, span))
        return number

    def arrival(self):
        self.recvs += 1
        return self.recvs - 1

    def copy(self, source, target, device, stage, arrival):
        pltpu.make_async_remote_copy(
            src_ref=source,
            dst_ref=target,
            send_sem=self.send.at[stage],
            recv_sem=self.recv.at[arrival],
            device_id=device,
            device_id_type=MESH,
        ).start()

    def arrived(self, arrival, span):
        pltpu.make_async_copy(span, span, self.recv.at[arrival]).wait()

    def close(self):
        for number, span in self.closing:
            pltpu.make_async_copy(span, span, self.send.at[number]).wait()


def place():
    x = lax.axis_index("x")
    return {"x": x // 2, "y": lax.axis_index("y"), "z": lax.axis_index("z"), "core": lax.rem(x, 2)}


def device_at(here, offsets):
    where = {}
    for axis, step in offsets:
        other = lax.rem(here[axis] + step, RING)
        where[axis] = other * 2 + here["core"] if axis == "x" else other
    return where


def partner(here):
    return {"x": here["x"] * 2 + 1 - here["core"]}


def group_offsets(axes):
    steps = list(itertools.product(range(RING), repeat=len(axes)))[1:]
    steps.sort(key=lambda step: -sum(min(s, RING - s) for s in step))
    return steps


def greet(here, groups):
    barrier = pltpu.get_barrier_semaphore()
    peers = {(("core", 1),): partner(here)}
    for axes in groups:
        for step in group_offsets(axes):
            key = tuple(sorted((axis, s) for axis, s in zip(axes, step) if s))
            peers[key] = device_at(here, key)
    for peer in peers.values():
        pl.semaphore_signal(barrier, inc=1, device_id=peer, device_id_type=MESH)
    return len(peers)


def shard_of(block, here, axes, step):
    for axis, s in zip(axes, step):
        block = block.part(lax.rem(here[axis] + s, RING) if s else here[axis], RING)
    return block


def buffer_shapes(half, levels):
    block = half(0)
    shapes = [block.shape(), block.shape()]
    for axes in levels:
        for _ in axes:
            block = block.part(0, RING)
        shapes.append((RING ** len(axes) - 1,) + block.shape())
    return shapes


def reduce_unit(here, levels, grad, half, buffers, out, sems, scale):
    core = here["core"]
    far = partner(here)
    from_pair, total = buffers[0], buffers[1]
    arrival = sems.arrival()
    sems.copy(grad, from_pair, far, sems.stage(from_pair), arrival)
    yield
    sems.arrived(arrival, from_pair)
    mine = half(core)
    total[...] += from_pair[...]
    base = Region(0, mine.rows, 0, mine.cols)
    bases = [base]
    for level, axes in enumerate(levels):
        slots = buffers[2 + level]
        steps = group_offsets(axes)
        stage, arrival = sems.stage(slots), sems.arrival()
        for slot, step in enumerate(steps):
            target = device_at(here, list(zip(axes, step)))
            sems.copy(shard_of(base, here, axes, step).at(total), slots.at[slot], target, stage, arrival)
        yield
        base = shard_of(base, here, axes, (0,) * len(axes))
        bases.append(base)
        sems.arrived(arrival, slots)
        result = base.load(total)
        for slot in range(len(steps)):
            result = result + slots[slot]
        if level + 1 < len(levels):
            base.store(total, result)
        else:
            base.moved(mine.row, mine.col).store(out, result * scale)
    for level in reversed(range(1, len(levels))):
        slots, axes = buffers[2 + level], levels[level]
        own = bases[level + 1].moved(mine.row, mine.col).at(out)
        stage, arrival = sems.stage(slots), sems.arrival()
        for step in group_offsets(axes):
            sems.copy(own, own, device_at(here, list(zip(axes, step))), stage, arrival)
        yield
        sems.arrived(arrival, slots)
    axes = levels[0]
    steps = group_offsets(axes)
    own = bases[1].moved(mine.row, mine.col).at(out)
    stage, arrivals = sems.stage(buffers[2]), [sems.arrival() for _ in steps]
    for step, arrival in zip(steps, arrivals):
        sems.copy(own, own, device_at(here, list(zip(axes, step))), stage, arrival)
    stage, last = sems.stage(from_pair), sems.arrival()
    sems.copy(own, own, far, stage, last)
    yield
    for step, arrival in reversed(list(zip(steps, arrivals))):
        back = tuple((RING - s) % RING for s in step)
        block = shard_of(bases[0], here, axes, back).moved(mine.row, mine.col).at(out)
        sems.arrived(arrival, block)
        sems.copy(block, block, far, stage, last)
    yield
    sems.arrived(last, from_pair)


def stages_of(levels):
    return 2 + 2 * len(levels)


def arrivals_of(levels):
    return stages_of(levels) - 1 + RING ** len(levels[0]) - 1


def tall(row, rows, apart):
    return lambda core: Region(row + core * apart, rows, 0, 256)


def wide(row, rows):
    return lambda core: Region(row, rows, core * 512, 512)


UNITS = (
    (DOWN2, tall(0, 512, 512), ORDERS[0]),
    (UP2, wide(0, 256), ORDERS[1]),
    (DOWN1, tall(0, 512, 512), ORDERS[2]),
    (UP1, wide(0, 128), ORDERS[1]),
    (UP1, wide(128, 128), ORDERS[2]),
    (IN, tall(0, 512, 1024), ORDERS[0]),
    (IN, tall(512, 256, 1024), ORDERS[1]),
    (IN, tall(768, 256, 1024), ORDERS[2]),
)

PLAN = (
    "c0", "c1", "c2", "c3", "bar", "o0", "u0", "m0", "c4", "o1", "u1", "m1",
    "c5", "u0", "o2", "u2", "m2", "c6", "u1", "o3", "o4", "u3", "u4", "m3",
    "m4", "u2", "c7", "u3", "u4", "o5", "u5", "o6", "u6", "o7", "u7", "m5",
    "m6", "m7", "c8", "u5", "u6", "u7",
)


def tiles():
    return [pl.ds(at, TILE) for at in range(0, ROWS, TILE)]


def step_kernel(scale, *refs):
    inputs, refs = refs[:7], refs[7:]
    dx, *outs = refs[:6]
    refs = refs[6:]
    x, g, w_in, w_up1, w_down1, w_up2, w_down2 = refs[:7]
    refs = refs[7:]
    mid, act_one, slope_one, hid_two, act_three, slope_three, d_pre3, d_hid2, d_pre1, d_mid = refs[:10]
    refs = refs[10:]
    grads, refs = refs[: len(UNITS)], refs[len(UNITS) :]
    buffers, (loads, send, recv) = refs[:-3], refs[-3:]
    here = place()
    peers = greet(here, sorted({axes for _, _, levels in UNITS for axes in levels}))

    core = here["core"]
    order = (1 - core, core)
    number = 0
    pending = []
    for source, target, axis in zip(inputs, refs_of(x, g, w_in, w_up1, w_down1, w_up2, w_down2), (1, None, 0, 1, 0, 1, 0)):
        size = target.shape[axis or 0] // (1 if axis is None else 2)
        for place_here, place_there in enumerate((0,) if axis is None else order):
            there, to = pl.ds(hinted(place_there * size, size), size), pl.ds(place_here * size, size)
            where = (there, to) if axis != 1 else ((slice(None), there), (slice(None), to))
            pending.append(pltpu.make_async_copy(source.at[where[0]], target.at[where[1]], loads.at[number]))
            number += 1
    for copy in pending:
        copy.start()

    def project():
        for copy in pending:
            copy.wait()
        for rows in tiles():
            mid[rows, :] = plain_product(x[rows, :], w_in[...]).astype(HALF)

    def expand(source, weight, act, slope):
        for rows in tiles():
            value, rate = gelu_pair(plain_product(source[rows, :], weight[...]).astype(HALF))
            act[rows, :] = value.astype(HALF)
            slope[rows, :] = rate

    def second():
        for rows in tiles():
            hid_two[rows, :] = (plain_product(act_one[rows, :], w_down1[...]) + mid[rows, :].astype(WIDE)).astype(HALF)

    def before_gelu(source, weight, slope, target):
        for rows in tiles():
            grad = times_transposed(source[rows, :], weight[...]).astype(HALF)
            target[rows, :] = (grad.astype(WIDE) * slope[rows, :]).astype(HALF)

    def before_layer(source, weight, skip, target):
        for rows in tiles():
            target[rows, :] = (times_transposed(source[rows, :], weight[...]) + skip[rows, :].astype(WIDE)).astype(HALF)

    def third():
        expand(hid_two, w_up2, act_three, slope_three)

    def leave():
        for place_here, place_there in enumerate(order):
            columns = pl.ds(hinted(place_there * 1024, 1024), 1024)
            for rows in tiles():
                dx[rows, columns] = times_transposed(d_mid[rows, :], w_in[pl.ds(place_here * 1024, 1024), :]).astype(HALF)

    stages = (
        project,
        lambda: expand(mid, w_up1, act_one, slope_one),
        second,
        third,
        lambda: before_gelu(g, w_down2, slope_three, d_pre3),
        lambda: before_layer(d_pre3, w_up2, g, d_hid2),
        lambda: before_gelu(d_hid2, w_down1, slope_one, d_pre1),
        lambda: before_layer(d_pre1, w_up1, d_hid2, d_mid),
        leave,
    )
    factors = {DOWN2: (act_three, g), UP2: (hid_two, d_pre3), DOWN1: (act_one, d_hid2), UP1: (mid, d_pre1), IN: (x, d_mid)}

    def gradient(unit, own):
        array, half, _ = UNITS[unit]
        first, other = factors[array]
        block = half(own)
        left = first[:, block.row : block.row + block.rows]
        right = other[:, block.col : block.col + block.cols]
        (totals if own else grads)[unit][...] = rows_contract(left, right)

    sems = Semaphores(send, recv)
    units, totals = [], []
    at = 0
    for array, half, levels in UNITS:
        count = len(buffer_shapes(half, levels))
        units.append(reduce_unit(here, levels, grads[len(units)], half, buffers[at : at + count], outs[array], sems, scale))
        totals.append(buffers[at + 1])
        at += count
    live = dict(enumerate(units))

    def advance(unit):
        if unit in live and next(live[unit], "done") == "done":
            del live[unit]

    for word in PLAN:
        if word == "bar":
            pl.semaphore_wait(pltpu.get_barrier_semaphore(), peers)
            continue
        kind, which = word[0], int(word[1:])
        if kind == "c":
            stages[which]()
        elif kind == "u":
            advance(which)
        else:
            gradient(which, 0 if kind == "o" else 1)
    while live:
        for unit in list(live):
            advance(unit)
    sems.close()


def refs_of(*refs):
    return refs


def fused_step(args, scale):
    vmem = pltpu.VMEM
    inputs = ((ROWS, 2048), (ROWS, 256), (2048, 256), (256, 1024), (1024, 256), (256, 1024), (1024, 256))
    scratch = [vmem(shape, HALF) for shape in inputs]
    scratch += [
        vmem((ROWS, 256), HALF),
        vmem((ROWS, 1024), HALF),
        vmem((ROWS, 1024), WIDE),
        vmem((ROWS, 256), HALF),
        vmem((ROWS, 1024), HALF),
        vmem((ROWS, 1024), WIDE),
        vmem((ROWS, 1024), HALF),
        vmem((ROWS, 256), HALF),
        vmem((ROWS, 1024), HALF),
        vmem((ROWS, 256), HALF),
    ]
    scratch += [vmem(half(0).shape(), WIDE) for _, half, _ in UNITS]
    for _, half, levels in UNITS:
        scratch += [vmem(shape, WIDE) for shape in buffer_shapes(half, levels)]
    scratch += [pltpu.SemaphoreType.DMA((13,))]
    scratch += [pltpu.SemaphoreType.DMA((sum(count(levels) for _, _, levels in UNITS),)) for count in (stages_of, arrivals_of)]
    outs = [jax.ShapeDtypeStruct((ROWS, 2048), HALF)] + [jax.ShapeDtypeStruct(shape, WIDE) for shape in SHAPES]

    def body(*refs):
        step_kernel(scale, *refs)

    return pl.pallas_call(
        body,
        out_shape=outs,
        in_specs=[pl.BlockSpec(memory_space=pltpu.HBM)] * 7,
        out_specs=[pl.BlockSpec(memory_space=pltpu.VMEM)] * 6,
        scratch_shapes=scratch,
        compiler_params=pltpu.CompilerParams(collective_id=0, has_side_effects=True, vmem_limit_bytes=40 * 1024 * 1024),
    )(*args)


def deliver(arrays):
    count = len(arrays)

    def body(*refs):
        copies = [pltpu.make_async_copy(refs[i], refs[count + i], refs[-1].at[i]) for i in range(count)]
        for copy in copies:
            copy.start()
        for copy in copies:
            copy.wait()

    return pl.pallas_call(
        body,
        out_shape=[jax.ShapeDtypeStruct(array.shape, array.dtype) for array in arrays],
        in_specs=[pl.BlockSpec(memory_space=pl.ANY)] * count,
        out_specs=[pl.BlockSpec(memory_space=pl.ANY)] * count,
        scratch_shapes=[pltpu.SemaphoreType.DMA((count,))],
        compiler_params=pltpu.CompilerParams(vmem_limit_bytes=1024 * 1024),
    )(*arrays)


def solution(mesh):
    batch_axes = ("z", "y", "x")
    scale = 1.0 / math.prod(mesh.shape.values())
    row_spec = P(batch_axes, None)
    full_spec = P(None, None)

    def device_step(*args):
        args = [pltpu.with_memory_space_constraint(arg, pltpu.HBM) for arg in args]
        return tuple(deliver(fused_step(args, scale)))

    return jax.shard_map(
        device_step,
        mesh=mesh,
        in_specs=(row_spec, row_spec, full_spec, full_spec, full_spec, full_spec, full_spec),
        out_specs=(row_spec, full_spec, full_spec, full_spec, full_spec, full_spec),
        check_vma=False,
    )
```
